8 devices in a mesh: dp: 1 (over z), tp: 8 (over y, x, core).
Axes of the slice: x: 2, y: 2, z: 1, core: 2. Of those that a mesh axis runs over, the one named last changes fastest.
Arguments:
- x_in: bfloat16 [1, 2048, 1536], P('dp', 'tp')
- y_grad: bfloat16 [1, 2048, 1536], P('dp', 'tp')
- ln_par: float32 [2, 4, 1536], replicated
- bias_d: float32 [2, 2, 1536], replicated
- w_qkv: bfloat16 [2, 1536, 3, 16, 96], P(None, None, None, 'tp')
- w_out: bfloat16 [2, 16, 96, 1536], P(None, 'tp')
- w_up: bfloat16 [2, 1536, 6144], P(None, None, 'tp')
- b_up: float32 [2, 6144], P(None, 'tp')
- w_down: bfloat16 [2, 6144, 1536], P(None, 'tp')
Outputs:
- output 1: bfloat16 [1, 2048, 1536], P('dp', 'tp')
- output 2: bfloat16 [1, 2048, 1536], P('dp', 'tp')
- output 3: float32 [2, 4, 1536], P('dp')
- output 4: float32 [2, 2, 1536], P('dp')
- output 5: bfloat16 [2, 1536, 3, 16, 96], P('dp', None, None, 'tp')
- output 6: bfloat16 [2, 16, 96, 1536], P('dp', 'tp')
- output 7: bfloat16 [2, 1536, 6144], P('dp', None, 'tp')
- output 8: float32 [2, 6144], P('dp', 'tp')
- output 9: bfloat16 [2, 6144, 1536], P('dp', 'tp')
All inputs are finite; a program needn't handle non-finite values.
Results may differ from the reference program's by a relative error of at most 0.02.
Values are sent between devices in bfloat16 or wider.
A program may use at most 1 GiB of HBM per device.

```python
import math
import jax
import jax.numpy as jnp
from jax import lax

N_BATCH = 1
SEQ_LEN = 2048
D_MODEL = 1536
N_HEADS = 16
HEAD_DIM = 96
FF_DIM = 6144
N_LAYERS = 2


def layer_norm(row_vals, ln_gain, ln_shift):
    mean_val = jnp.mean(row_vals, axis=-1, keepdims=True)
    centered = row_vals - mean_val
    var_val = jnp.mean(centered * centered, axis=-1, keepdims=True)
    return centered * lax.rsqrt(var_val + 1e-5) * ln_gain + ln_shift


def setup_inputs(seed: int = 0, part: int = 0) -> dict:
    part_key = jax.random.fold_in(jax.random.key(seed), part)
    part_list = jax.random.split(part_key, 3)
    key_list = jax.random.split(jax.random.key(seed + 1), 7)
    act_shape = (N_BATCH, SEQ_LEN, D_MODEL)
    token_scale = jax.random.uniform(part_list[0], (N_BATCH, SEQ_LEN, 1), jnp.float32, 0.5, 1.5)
    x_in = (jax.random.normal(part_list[1], act_shape, jnp.float32) * token_scale).astype(jnp.bfloat16)
    y_grad = jax.random.normal(part_list[2], act_shape, jnp.float32).astype(jnp.bfloat16)
    ln_base = jnp.array([1.0, 0.0, 1.0, 0.0], jnp.float32)[None, :, None]
    ln_par = ln_base + 0.2 * jax.random.normal(key_list[0], (N_LAYERS, 4, D_MODEL), jnp.float32)
    bias_d = 0.2 * jax.random.normal(key_list[1], (N_LAYERS, 2, D_MODEL), jnp.float32)
    qk_gain = (math.log(SEQ_LEN) / 2.0) ** 0.25
    qkv_gain = jnp.array([qk_gain, qk_gain, 1.0], jnp.float32)[None, None, :, None, None] * D_MODEL ** -0.5
    w_qkv = (jax.random.normal(key_list[2], (N_LAYERS, D_MODEL, 3, N_HEADS, HEAD_DIM), jnp.float32) * qkv_gain).astype(jnp.bfloat16)
    out_gain = 0.3 * SEQ_LEN ** 0.25 * D_MODEL ** -0.5
    w_out = (jax.random.normal(key_list[3], (N_LAYERS, N_HEADS, HEAD_DIM, D_MODEL), jnp.float32) * out_gain).astype(jnp.bfloat16)
    w_up = (jax.random.normal(key_list[4], (N_LAYERS, D_MODEL, FF_DIM), jnp.float32) * D_MODEL ** -0.5).astype(jnp.bfloat16)
    b_up = 0.5 * jax.random.normal(key_list[5], (N_LAYERS, FF_DIM), jnp.float32)
    w_down = (jax.random.normal(key_list[6], (N_LAYERS, FF_DIM, D_MODEL), jnp.float32) * FF_DIM ** -0.5).astype(jnp.bfloat16)
    return dict(x_in=x_in, y_grad=y_grad, ln_par=ln_par, bias_d=bias_d, w_qkv=w_qkv, w_out=w_out, w_up=w_up, b_up=b_up, w_down=w_down)


def head_attention(qkv_head):
    q_head = qkv_head[:, 0].astype(jnp.float32)
    k_head = qkv_head[:, 1].astype(jnp.float32)
    v_head = qkv_head[:, 2].astype(jnp.float32)
    scores = jnp.dot(q_head, k_head.T) * (HEAD_DIM ** -0.5)
    positions = jnp.arange(SEQ_LEN)
    causal = positions[:, None] >= positions[None, :]
    scores = jnp.where(causal, scores, -1e30)
    prob_bf = jax.nn.softmax(scores, axis=-1).astype(jnp.bfloat16)
    return jnp.dot(prob_bf.astype(jnp.float32), v_head).astype(jnp.bfloat16)


def attention_all(qkv_vals):
    per_head = jnp.transpose(qkv_vals, (0, 3, 1, 2, 4)).reshape(N_BATCH * N_HEADS, SEQ_LEN, 3, HEAD_DIM)
    head_out = lax.map(jax.checkpoint(head_attention), per_head)
    return jnp.transpose(head_out.reshape(N_BATCH, N_HEADS, SEQ_LEN, HEAD_DIM), (0, 2, 1, 3))


def block_forward(residual, layer_w):
    ln_vals, bias_vals, w_qkv, w_out, w_up, b_up, w_down = layer_w
    h_one = layer_norm(residual, ln_vals[0], ln_vals[1]).astype(jnp.bfloat16)
    qkv_vals = jnp.einsum('bsd,dche->bsche', h_one.astype(jnp.float32), w_qkv.astype(jnp.float32)).astype(jnp.bfloat16)
    attn_vals = attention_all(qkv_vals)
    attn_out = jnp.einsum('bshe,hed->bsd', attn_vals.astype(jnp.float32), w_out.astype(jnp.float32))
    residual = residual + attn_out + bias_vals[0]
    h_two = layer_norm(residual, ln_vals[2], ln_vals[3]).astype(jnp.bfloat16)
    pre_act = jnp.einsum('bsd,df->bsf', h_two.astype(jnp.float32), w_up.astype(jnp.float32)) + b_up
    act_vals = jax.nn.gelu(pre_act, approximate=True).astype(jnp.bfloat16)
    mlp_out = jnp.einsum('bsf,fd->bsd', act_vals.astype(jnp.float32), w_down.astype(jnp.float32))
    return residual + mlp_out + bias_vals[1]


def reference(x_in, y_grad, ln_par, bias_d, w_qkv, w_out, w_up, b_up, w_down):
    weights = (ln_par, bias_d, w_qkv, w_out, w_up, b_up, w_down)

    def forward(x_vals, layer_stack):
        def scan_body(residual, layer_w):
            return block_forward(residual, layer_w), None
        final_res, _ = lax.scan(scan_body, x_vals.astype(jnp.float32), layer_stack)
        return final_res

    final_res, pullback = jax.vjp(forward, x_in, weights)
    x_ct, w_ct = pullback(y_grad.astype(jnp.float32))
    return (final_res.astype(jnp.bfloat16), x_ct, w_ct[0], w_ct[1], w_ct[2], w_ct[3], w_ct[4], w_ct[5], w_ct[6])
```

```python
import functools
import math

import jax
import jax.numpy as jnp
from jax import lax
from jax.experimental import pallas as pl
from jax.experimental.pallas import tpu as pltpu
from jax.sharding import PartitionSpec as P

MESH = pl.DeviceIdType.MESH
BF16 = jnp.bfloat16
F32 = jnp.float32
LOG2E = math.log2(math.e)
VMEM_LIMIT = 60 * 1024 * 1024
LANES = 128


def dot_nn(a, b):
    return lax.dot_general(a, b, (((1,), (0,)), ((), ())), preferred_element_type=F32)


def dot_nt(a, b):
    return lax.dot_general(a, b, (((1,), (1,)), ((), ())), preferred_element_type=F32)


def dot_tn(a, b):
    return lax.dot_general(a, b, (((0,), (0,)), ((), ())), preferred_element_type=F32)


def attn_fwd_kernel(scale, n_q, q_ref, k_ref, v_ref, a_ref, lse_ref):
    blk = q_ref.shape[0]
    coef = scale * LOG2E
    row = lax.broadcasted_iota(jnp.int32, (blk, blk), 0)
    col = lax.broadcasted_iota(jnp.int32, (blk, blk), 1)

    def variant(i):
        q = q_ref[...]
        parts = []
        for j in range(i + 1):
            s = dot_nt(q, k_ref[j * blk:(j + 1) * blk, :])
            if j == i:
                s = jnp.where(row >= col, s, -1e30)
            parts.append(s)
        top = parts[0]
        for s in parts[1:]:
            top = jnp.maximum(top, s)
        top = jnp.max(top, axis=-1, keepdims=True) * coef
        parts = [jnp.exp2(s * coef - top) for s in parts]
        total = parts[0]
        for e in parts[1:]:
            total = total + e
        total = jnp.sum(total, axis=-1, keepdims=True)
        inv = 1.0 / total
        out = None
        for j, e in enumerate(parts):
            o = dot_nn((e * inv).astype(BF16), v_ref[j * blk:(j + 1) * blk, :])
            out = o if out is None else out + o
        a_ref[...] = out.astype(BF16)
        lse = jnp.broadcast_to(top + jnp.log2(total), (blk, 128))
        lse_ref[0] = jnp.transpose(lse)[0:1, :]

    for i in range(n_q):
        pl.when(pl.program_id(1) == i)(functools.partial(variant, i))


def attention_forward(qkv, head_dim, n_heads):
    seq = qkv.shape[0]
    blk = 512
    n_q = seq // blk
    return pl.pallas_call(
        functools.partial(attn_fwd_kernel, head_dim ** -0.5, n_q),
        grid=(n_heads, n_q),
        in_specs=[pl.BlockSpec((blk, 128), lambda h, i: (i, h)),
                  pl.BlockSpec((seq, 128), lambda h, i: (0, n_heads + h)),
                  pl.BlockSpec((seq, 128), lambda h, i: (0, 2 * n_heads + h))],
        out_specs=[pl.BlockSpec((blk, 128), lambda h, i: (i, h)),
                   pl.BlockSpec((1, 1, blk), lambda h, i: (h, 0, i))],
        out_shape=[jax.ShapeDtypeStruct((seq, n_heads * 128), BF16),
                   jax.ShapeDtypeStruct((n_heads, 1, seq), F32)],
        compiler_params=pltpu.CompilerParams(dimension_semantics=("arbitrary", "arbitrary"), vmem_limit_bytes=40 * 1024 * 1024),
        cost_estimate=pl.CostEstimate(flops=4 * seq * seq * 128, bytes_accessed=8 * seq * 256, transcendentals=seq * seq),
        name="attn_fwd",
    )(qkv, qkv, qkv)


def attn_bwd_kernel(scale, n_q, q_ref, k_ref, v_ref, a_ref, da_ref, lse_ref, dq_ref, dk_ref, dv_ref, dk_acc, dv_acc):
    blk = q_ref.shape[0]
    coef = scale * LOG2E
    key = lax.broadcasted_iota(jnp.int32, (blk, blk), 0)
    qry = lax.broadcasted_iota(jnp.int32, (blk, blk), 1)

    def variant(i):
        q = q_ref[...]
        da = da_ref[...]
        lse = lse_ref[0]
        row_dot = jnp.sum(jnp.transpose(da.astype(F32) * a_ref[...].astype(F32)), axis=0, keepdims=True)
        dq = None
        for j in range(i, -1, -1):
            rows = slice(j * blk, (j + 1) * blk)
            k = k_ref[rows, :]
            p = jnp.exp2(dot_nt(k, q) * coef - lse)
            if j == i:
                p = jnp.where(qry >= key, p, 0.0)
            dv = dot_nn(p.astype(BF16), da)
            ds = (p * (dot_nt(v_ref[rows, :], da) - row_dot)).astype(BF16)
            dk = dot_nn(ds, q)
            if j == i:
                dv_acc[rows, :] = dv
                dk_acc[rows, :] = dk
            else:
                dv_acc[rows, :] += dv
                dk_acc[rows, :] += dk
            d = dot_tn(ds, k)
            dq = d if dq is None else dq + d
        dq_ref[...] = (dq * scale).astype(BF16)

    for i in range(n_q):
        pl.when(pl.program_id(1) == i)(functools.partial(variant, i))

    @pl.when(pl.program_id(1) == n_q - 1)
    def _():
        dk_ref[...] = (dk_acc[...] * scale).astype(BF16)
        dv_ref[...] = dv_acc[...].astype(BF16)


def attention_backward(qkv, attn, d_attn, lse, head_dim, n_heads):
    seq = qkv.shape[0]
    blk = 512
    n_q = seq // blk
    row = pl.BlockSpec((blk, 128), lambda h, i: (i, h))
    full = pl.BlockSpec((seq, 128), lambda h, i: (0, h))
    shape = jax.ShapeDtypeStruct((seq, n_heads * 128), BF16)
    return pl.pallas_call(
        functools.partial(attn_bwd_kernel, head_dim ** -0.5, n_q),
        grid=(n_heads, n_q),
        in_specs=[row,
                  pl.BlockSpec((seq, 128), lambda h, i: (0, n_heads + h)),
                  pl.BlockSpec((seq, 128), lambda h, i: (0, 2 * n_heads + h)),
                  row, row,
                  pl.BlockSpec((1, 1, blk), lambda h, i: (h, 0, i))],
        out_specs=[row, full, full],
        out_shape=[shape, shape, shape],
        scratch_shapes=[pltpu.VMEM((seq, 128), F32), pltpu.VMEM((seq, 128), F32)],
        compiler_params=pltpu.CompilerParams(dimension_semantics=("arbitrary", "arbitrary"), vmem_limit_bytes=40 * 1024 * 1024),
        cost_estimate=pl.CostEstimate(flops=10 * seq * seq * 128, bytes_accessed=16 * seq * 256, transcendentals=seq * seq),
        name="attn_bwd",
    )(qkv, qkv, qkv, attn, d_attn, lse)


class Place:
    def __init__(self):
        t = lax.axis_index("tp")
        self.me = t
        self.dc = 1 - 2 * (t % 2)
        self.dx = 2 - 4 * ((t // 2) % 2)
        self.dy = 4 - 8 * (t // 4)
        self.partner = t + self.dc
        self.xn = t + self.dx
        self.yn = t + self.dy


def barrier(pos):
    sem = pltpu.get_barrier_semaphore()
    for peer in (pos.partner, pos.xn, pos.yn):
        pl.semaphore_signal(sem, inc=1, device_id={"tp": peer}, device_id_type=MESH)
    pl.semaphore_wait(sem, 3)


def rdma(src, dst, sems, idx, peer):
    send, recv = sems
    return pltpu.make_async_remote_copy(src_ref=src, dst_ref=dst, send_sem=send.at[idx], recv_sem=recv.at[idx],
                                        device_id={"tp": peer}, device_id_type=MESH)


def rs_scratch(rows, width):
    half = rows // 2
    return dict(
        rs_snd=pltpu.VMEM((4, rows, width), BF16), rs_rcv=pltpu.VMEM((4, rows, width), BF16),
        rs_sum=pltpu.VMEM((4, rows, width), F32), rs_out=pltpu.VMEM((3, rows, width), BF16),
        rs_in=pltpu.VMEM((6, half, width), BF16),
        rs_psend=pltpu.SemaphoreType.DMA((4,)), rs_precv=pltpu.SemaphoreType.DMA((4,)),
        rs_send=pltpu.SemaphoreType.DMA((6,)), rs_recv=pltpu.SemaphoreType.DMA((6,)))


def reduce_scatter(pos, r, produce, rows, width, n_chunk=3):
    half = rows // 2
    top, low = pl.ds(0, half), pl.ds(half, half)
    wide = width // n_chunk
    psem = (r.rs_psend, r.rs_precv)
    isem = (r.rs_send, r.rs_recv)

    def dest(k):
        return pos.me + (1 - k // 2) * pos.dx + (1 - k % 2) * pos.dy

    def to_partner(k):
        return rdma(r.rs_snd.at[k], r.rs_rcv.at[k], psem, k, pos.partner)

    def first(k, carry):
        block = dest(k) + pos.dc
        for c in range(n_chunk):
            cols = pl.ds(c * wide, wide)
            r.rs_snd[k, :, cols] = produce(block, cols).astype(BF16)
        to_partner(k).start()
        return carry

    lax.fori_loop(0, 4, first, 0)

    diag_x = rdma(r.rs_out.at[0, top], r.rs_in.at[0], isem, 0, pos.xn)
    diag_y = rdma(r.rs_out.at[0, low], r.rs_in.at[1], isem, 1, pos.yn)
    x_top = rdma(r.rs_out.at[1, top], r.rs_in.at[2], isem, 2, pos.xn)
    x_low = rdma(r.rs_out.at[1, low], r.rs_in.at[3], isem, 3, pos.xn)
    y_top = rdma(r.rs_out.at[2, top], r.rs_in.at[4], isem, 4, pos.yn)
    y_low = rdma(r.rs_out.at[2, low], r.rs_in.at[5], isem, 5, pos.yn)

    def second(k, carry):
        block = dest(k)
        to_partner(k).wait_recv()
        for c in range(n_chunk):
            cols = pl.ds(c * wide, wide)
            total = produce(block, cols) + r.rs_rcv[k, :, cols].astype(F32)
            r.rs_sum[k, :, cols] = total

            @pl.when(k < 3)
            def _():
                r.rs_out[k, :, cols] = r.rs_sum[k, :, cols].astype(BF16)

        @pl.when(k == 0)
        def _():
            diag_x.start()
            diag_y.start()

        @pl.when(k == 1)
        def _():
            x_top.start()

        @pl.when(k == 2)
        def _():
            y_low.start()

        return carry

    lax.fori_loop(0, 4, second, 0)

    diag_y.wait_recv()
    diag_x.wait_recv()

    def add_relay(slot, src, part):
        def body(i, carry):
            rr = pl.ds(pl.multiple_of(i * 16, 16), 16)
            at = pl.ds(pl.multiple_of(part * half + i * 16, 16), 16)
            r.rs_out[slot, at, :] = (r.rs_sum[slot, at, :] + r.rs_in[src, rr, :].astype(F32)).astype(BF16)
            return carry

        lax.fori_loop(0, half // 16, body, 0)

    add_relay(2, 0, 0)
    y_top.start()
    add_relay(1, 1, 1)
    x_low.start()

    x_top.wait_recv()
    y_low.wait_recv()
    y_top.wait_recv()
    x_low.wait_recv()

    def finish():
        for k in range(4):
            to_partner(k).wait_send()
        for copy in (diag_x, diag_y, x_top, x_low, y_top, y_low):
            copy.wait_send()

    return finish


def rs_rows(r, half, start, count):
    at = pl.ds(start, count)
    part = start // half
    inner = pl.ds(pl.multiple_of(start - part * half, count), count)
    return (r.rs_sum[3, at, :] + r.rs_in[2 + part, inner, :].astype(F32)) + r.rs_in[4 + part, inner, :].astype(F32)


def ag_scratch(seq, width):
    return dict(h_vm=pltpu.VMEM((seq, width), BF16),
                ag_send=pltpu.SemaphoreType.DMA((13,)), ag_recv=pltpu.SemaphoreType.DMA((13,)),
                h_out=pltpu.SemaphoreType.DMA((8,)))


def all_gather(pos, r, consume, rows, h_hbm, streams):
    half = rows // 2
    sems = (r.ag_send, r.ag_recv)

    def piece(owner, part):
        return r.h_vm.at[pl.ds(pl.multiple_of(owner * rows + part * half, half), half)]

    def whole(owner):
        return r.h_vm.at[pl.ds(pl.multiple_of(owner * rows, rows), rows)]

    def copy(ref, idx, peer):
        return rdma(ref, ref, sems, idx, peer)

    me, xn, yn = pos.me, pos.xn, pos.yn
    dn = me + pos.dx + pos.dy
    own_p = copy(whole(me), 0, pos.partner)
    own_xa = copy(piece(me, 0), 1, xn)
    own_xb = copy(piece(me, 1), 2, xn)
    own_ya = copy(piece(me, 0), 3, yn)
    own_yb = copy(piece(me, 1), 4, yn)
    relay_y = copy(piece(xn, 0), 5, yn)
    relay_x = copy(piece(yn, 1), 6, xn)
    fwd_xa = copy(piece(xn, 0), 7, pos.partner)
    fwd_xb = copy(piece(xn, 1), 8, pos.partner)
    fwd_ya = copy(piece(yn, 0), 9, pos.partner)
    fwd_yb = copy(piece(yn, 1), 10, pos.partner)
    fwd_da = copy(piece(dn, 0), 11, pos.partner)
    fwd_db = copy(piece(dn, 1), 12, pos.partner)
    own_xa.start()
    own_yb.start()
    own_xb.start()
    own_ya.start()
    own_p.start()

    def out_copies(s, block):
        at = pl.ds(pl.multiple_of(block * rows, rows), rows)
        made = [pltpu.make_async_copy(r.h_vm.at[at], h_hbm.at[at], r.h_out.at[s])]
        for src, dst, sem in streams:
            made.append(pltpu.make_async_copy(src.at[at], dst.at[at], sem.at[s]))
        return made

    def block_of(s):
        return me + (s % 2) * pos.dc + ((s // 2) % 2) * pos.dx + (s // 4) * pos.dy

    def step(s, carry):
        @pl.when(s == 1)
        def _():
            own_p.wait_recv()

        @pl.when(s == 2)
        def _():
            own_xa.wait_recv()
            relay_y.start()
            fwd_xa.start()
            own_yb.wait_recv()
            relay_x.start()
            fwd_yb.start()
            own_xb.wait_recv()
            fwd_xb.start()

        @pl.when(s == 3)
        def _():
            own_ya.wait_recv()
            fwd_ya.start()
            fwd_xa.wait_recv()
            fwd_xb.wait_recv()

        @pl.when(s == 5)
        def _():
            fwd_ya.wait_recv()
            fwd_yb.wait_recv()

        @pl.when(s == 6)
        def _():
            relay_y.wait_recv()
            fwd_da.start()
            relay_x.wait_recv()
            fwd_db.start()

        @pl.when(s == 7)
        def _():
            fwd_da.wait_recv()
            fwd_db.wait_recv()

        block = block_of(s)
        consume(block)
        for c in out_copies(s, block):
            c.start()
        return carry

    lax.fori_loop(0, 8, step, 0)

    def finish():
        for c in (own_p, own_xa, own_xb, own_ya, own_yb, relay_y, relay_x, fwd_xa, fwd_xb, fwd_ya, fwd_yb, fwd_da, fwd_db):
            c.wait_send()

        def drain(s, carry):
            for c in out_copies(s, block_of(s)):
                c.wait()
            return carry

        lax.fori_loop(0, 8, drain, 0)

    return finish


class Refs:
    pass


def comm_call(body, ins, outs, scratch, cid, name, flops):
    in_names, out_names, scr_names = list(ins), list(outs), list(scratch)
    any_spec, vmem_spec = pl.BlockSpec(memory_space=pl.ANY), pl.BlockSpec(memory_space=pltpu.VMEM)
    arrays, in_specs = [], []
    for key in in_names:
        val = ins[key]
        in_specs.append(any_spec if isinstance(val, tuple) else vmem_spec)
        arrays.append(val[0] if isinstance(val, tuple) else val)

    def kernel(*refs):
        r = Refs()
        for key, ref in zip(in_names + out_names + scr_names, refs):
            setattr(r, key, ref)
        body(r)

    result = pl.pallas_call(
        kernel,
        in_specs=in_specs,
        out_specs=[any_spec if outs[key][2] else vmem_spec for key in out_names],
        out_shape=[jax.ShapeDtypeStruct(outs[key][0], outs[key][1]) for key in out_names],
        scratch_shapes=[scratch[key] for key in scr_names],
        compiler_params=pltpu.CompilerParams(collective_id=cid, has_side_effects=True, vmem_limit_bytes=VMEM_LIMIT),
        cost_estimate=pl.CostEstimate(flops=flops, bytes_accessed=30_000_000, transcendentals=0),
        name=name,
    )(*arrays)
    return dict(zip(out_names, result))


def fold8(vals):
    out = vals[0:8]
    for i in range(8, vals.shape[0], 8):
        out = out + vals[i:i + 8]
    return out


def unit(cid, name, seq, width, *, lhs=None, weight=None, weight_t=False, local=None, local_in=None, tail=None, consume=None,
         cons_in=None, cons_out=None, cons_acc=None):
    rows = seq // 8
    half = rows // 2
    lhs, weight = lhs or [], weight or []
    cons_in, cons_out, cons_acc = cons_in or {}, cons_out or {}, cons_acc or {}
    ins, scratch, outs = {}, {}, {}
    loads = []
    for i, (a, w) in enumerate(zip(lhs, weight)):
        for tag, arr in ((f"lhs{i}", a), (f"w{i}", w)):
            ins[tag + "_h"] = (arr,)
            scratch[tag] = pltpu.VMEM(arr.shape, arr.dtype)
            loads.append(tag)
    n_prod = len(loads)
    for tag, arr in cons_in.items():
        ins[tag + "_h"] = (arr,)
        scratch[tag] = pltpu.VMEM(arr.shape, arr.dtype)
        loads.append(tag)
    ins.update(local_in or {})
    for tag, (shape, dtype) in (tail or {}).items():
        outs[tag] = (shape, dtype, False)
    if lhs:
        scratch.update(rs_scratch(rows, width))
    if consume:
        scratch.update(ag_scratch(seq, width))
        outs["h_all"] = ((seq, width), BF16, True)
        for tag, (cols, dtype) in cons_out.items():
            outs[tag + "_h"] = ((seq, cols), dtype, True)
            scratch[tag] = pltpu.VMEM((seq, cols), dtype)
            scratch[tag + "_s"] = pltpu.SemaphoreType.DMA((8,))
        for tag, (shape, dtype) in cons_acc.items():
            outs[tag] = (shape, dtype, False)
    scratch["load_sem"] = pltpu.SemaphoreType.DMA((max(len(loads), 1),))

    def body(r):
        pos = Place()
        load = [pltpu.make_async_copy(getattr(r, tag + "_h"), getattr(r, tag), r.load_sem.at[i]) for i, tag in enumerate(loads)]
        for c in load:
            c.start()
        barrier(pos)
        finish_rs = None
        get_rows = None
        if lhs:
            for c in load[:n_prod]:
                c.wait()

            def produce(block, cols):
                at = pl.ds(pl.multiple_of(block * rows, rows), rows)
                total = None
                for i in range(len(lhs)):
                    a, w = getattr(r, f"lhs{i}"), getattr(r, f"w{i}")
                    part = dot_nt(a[at, :], w[cols, :]) if weight_t else dot_nn(a[at, :], w[:, cols])
                    total = part if total is None else total + part
                return total

            finish_rs = reduce_scatter(pos, r, produce, rows, width)
            get_rows = functools.partial(rs_rows, r, half)
        local(r, pos, get_rows)
        if consume:
            for c in load[n_prod:]:
                c.wait()
            for tag in cons_acc:
                ref = getattr(r, tag)
                ref[...] = jnp.zeros_like(ref)
            streams = [(getattr(r, tag), getattr(r, tag + "_h"), getattr(r, tag + "_s")) for tag in cons_out]

            def run(block):
                consume(r, pl.ds(pl.multiple_of(block * rows, rows), rows))

            finish_ag = all_gather(pos, r, run, rows, r.h_all, streams)
            finish_ag()
        if finish_rs:
            finish_rs()

    flops = 2 * seq * width * (sum(a.shape[1] for a in lhs) + sum(c for c, _ in cons_out.values())) + 100_000
    if "small" in (local_in or {}):
        scratch.update(sm_rcv=pltpu.VMEM((3,) + local_in["small"].shape, F32), sm_snd=pltpu.VMEM((3,) + local_in["small"].shape, F32),
                       sm_send=pltpu.SemaphoreType.DMA((3,)), sm_recv=pltpu.SemaphoreType.DMA((3,)))
    return comm_call(body, ins, outs, scratch, cid, name, flops)


STEP_ROWS = 16


def normalize(res):
    mean = jnp.mean(res, axis=-1, keepdims=True)
    centered = res - mean
    var = jnp.mean(centered * centered, axis=-1, keepdims=True)
    rstd = lax.rsqrt(var + 1e-5)
    return centered * rstd, rstd


def local_forward(rows, with_sum, with_h):
    def run(r, pos, get_rows):
        base = pos.me * rows

        def step(i, carry):
            at = pl.multiple_of(i * STEP_ROWS, STEP_ROWS)
            here = pl.ds(at, STEP_ROWS)
            res = r.res[here, :].astype(F32)
            if with_sum:
                res = (res + get_rows(at, STEP_ROWS)) + r.ln[2:, :]
                r.res_out[here, :] = res.astype(r.res_out.dtype)
            if with_h:
                xhat, _ = normalize(res)
                r.h_vm[pl.ds(pl.multiple_of(base + at, STEP_ROWS), STEP_ROWS), :] = (
                    xhat * r.ln[0:1, :] + r.ln[1:2, :]).astype(BF16)
            return carry

        lax.fori_loop(0, rows // STEP_ROWS, step, 0)

    return run


def local_backward(rows, last, n_small=0):
    def run(r, pos, get_rows):
        base = pos.me * rows
        width = r.ln.shape[-1]

        def step(i, carry):
            d_gain, d_shift, d_bias = carry
            at = pl.multiple_of(i * STEP_ROWS, STEP_ROWS)
            here = pl.ds(at, STEP_ROWS)
            d_h = get_rows(at, STEP_ROWS)
            xhat, rstd = normalize(r.res[here, :].astype(F32))
            d_gain = d_gain + fold8(d_h * xhat)
            d_shift = d_shift + fold8(d_h)
            d_hat = d_h * r.ln[0:1, :]
            m_one = jnp.mean(d_hat, axis=-1, keepdims=True)
            m_two = jnp.mean(d_hat * xhat, axis=-1, keepdims=True)
            d_out = r.d_res[here, :].astype(F32) + rstd * (d_hat - m_one - xhat * m_two)
            d_bias = d_bias + fold8(d_out)
            r.d_out[here, :] = d_out.astype(r.d_out.dtype)
            if not last:
                r.h_vm[pl.ds(pl.multiple_of(base + at, STEP_ROWS), STEP_ROWS), :] = d_out.astype(BF16)
            return d_gain, d_shift, d_bias

        zero = jnp.zeros((8, width), F32)
        d_gain, d_shift, d_bias = lax.fori_loop(0, rows // STEP_ROWS, step, (zero, zero, zero))
        if not last:
            r.sums[0:1, :] = jnp.sum(d_gain, axis=0, keepdims=True)
            r.sums[1:2, :] = jnp.sum(d_shift, axis=0, keepdims=True)
            r.sums[2:3, :] = jnp.sum(d_bias, axis=0, keepdims=True)
            return
        r.sm_snd[0] = r.small[...]
        r.sm_snd[0, 0:1, :] = jnp.sum(d_gain, axis=0, keepdims=True)
        r.sm_snd[0, 1:2, :] = jnp.sum(d_shift, axis=0, keepdims=True)
        sems = (r.sm_send, r.sm_recv)
        copies = []
        for i, peer in enumerate((pos.partner, pos.xn, pos.yn)):
            c = rdma(r.sm_snd.at[i], r.sm_rcv.at[i], sems, i, peer)
            c.start()
            c.wait_recv()
            copies.append(c)
            total = r.sm_snd[i] + r.sm_rcv[i]
            if i < 2:
                r.sm_snd[i + 1] = total
            else:
                r.small_out[...] = total
        for c in copies:
            c.wait_send()

    return run


GELU_C = math.sqrt(2.0 / math.pi)


def gelu_pair(x):
    sq = x * x
    t = jnp.tanh(GELU_C * x * (1.0 + 0.044715 * sq))
    half = 0.5 * (1.0 + t)
    grad = half + (0.5 * GELU_C) * x * (1.0 - t * t) * (1.0 + (3 * 0.044715) * sq)
    return x * half, grad


def consume_qkv(r, at):
    h = r.h_vm[at, :]
    for c in range(0, r.qkv.shape[1], 256):
        cols = pl.ds(c, 256)
        r.qkv[at, cols] = dot_nt(h, r.wqkv[cols, :]).astype(BF16)


def consume_up(r, at):
    h = r.h_vm[at, :]
    for c in range(0, r.act.shape[1], 256):
        cols = pl.ds(c, 256)
        act, grad = gelu_pair(dot_nn(h, r.w_up[:, cols]) + r.b_up[:, cols])
        r.act[at, cols] = act.astype(BF16)
        r.gel[at, cols] = grad


def consume_up_down(r, at):
    h = r.h_vm[at, :]
    dy = r.dy[at, :]
    for c in range(0, r.act.shape[1], 256):
        cols = pl.ds(c, 256)
        act, grad = gelu_pair(dot_nn(h, r.w_up[:, cols]) + r.b_up[:, cols])
        r.act[at, cols] = act.astype(BF16)
        d_pre = dot_nt(dy, r.w_down[cols, :]) * grad
        r.d_bup[:, cols] += fold8(d_pre)
        r.d_pre[at, cols] = d_pre.astype(BF16)


def consume_dpre(r, at):
    d = r.h_vm[at, :]
    for c in range(0, r.d_pre.shape[1], 256):
        cols = pl.ds(c, 256)
        d_pre = dot_nt(d, r.w_down[cols, :]) * r.gel[at, cols]
        r.d_bup[:, cols] += fold8(d_pre)
        r.d_pre[at, cols] = d_pre.astype(BF16)


def consume_dattn(r, at):
    r.d_attn[at, :] = dot_nt(r.h_vm[at, :], r.w_out[...]).astype(BF16)


def spec(text):
    return P(*[name if name in ("dp", "tp") else None for name in text.split()])


def stack_all(groups):
    return [jnp.stack(group) for group in groups]


def solution(mesh):
    def device_step(x_loc, dy_loc, ln_par, bias_d, w_qkv, w_out, w_up, b_up, w_down):
        (x_in,), (dy,) = x_loc, dy_loc
        rows, width = x_in.shape
        seq = rows * mesh.shape['tp']
        n_heads, head_dim = w_qkv.shape[-2:]
        ff = w_up.shape[-1]
        lanes = n_heads * LANES

        def pad_heads(w):
            flat = w.reshape((-1, head_dim, width))
            return jnp.concatenate([flat, jnp.zeros((flat.shape[0], LANES - head_dim, width), BF16)], axis=1).reshape((-1, width))

        wqkv_t = [pad_heads(jnp.moveaxis(w, 0, -1)) for w in w_qkv]
        wo = [pad_heads(w) for w in w_out]
        parts = [w.reshape((-1, lanes, width)) for w in wqkv_t]
        (up_a, up_b), (down_a, down_b), (wq_a, wq_b), (wo_a, wo_b) = w_up, w_down, wqkv_t, wo
        bup_a, bup_b = jnp.split(b_up, 2)
        (gain_a, shift_a, gain_b, shift_b), (gain_c, shift_c, gain_d, shift_d) = ln_par
        (bias_a, bias_b), (bias_c, bias_d2) = bias_d
        part_a, part_b = [list(w) for w in parts]

        f32_rows = ((rows, width), F32)
        bf_rows = ((rows, width), BF16)
        sums = ((8, width), F32)
        keep = dict(res_out=f32_rows)
        back = dict(d_out=f32_rows, sums=sums)
        qkv_out = dict(qkv=(len(wq_a), BF16))
        dattn_out = dict(d_attn=(lanes, BF16))
        bup_acc = dict(d_bup=((8, ff), F32))
        enter, middle, leave = local_forward(rows, False, True), local_forward(rows, True, True), local_forward(rows, True, False)
        backward = local_backward(rows, False)

        u0 = unit(0, "ag_qkv0", seq, width, local=enter, local_in=dict(res=x_in, ln=jnp.stack([gain_a, shift_a])),
                  consume=consume_qkv, cons_in=dict(wqkv=wq_a), cons_out=qkv_out)
        qkv_a = u0["qkv_h"]
        dy_dep, _ = lax.optimization_barrier((dy, qkv_a))
        dy_all = lax.all_gather(dy_dep, 'tp', axis=0, tiled=True)

        attn_a, lse_a = attention_forward(qkv_a, head_dim, n_heads)
        u1 = unit(1, "out_up0", seq, width, lhs=[attn_a], weight=[wo_a], local=middle, tail=keep,
                  local_in=dict(res=x_in, ln=jnp.stack([gain_b, shift_b, bias_a])), consume=consume_up,
                  cons_in=dict(w_up=up_a, b_up=bup_a), cons_out=dict(act=(ff, BF16), gel=(ff, F32)))
        u2 = unit(2, "down_qkv1", seq, width, lhs=[u1["act_h"]], weight=[down_a], local=middle, tail=keep,
                  local_in=dict(res=u1["res_out"], ln=jnp.stack([gain_c, shift_c, bias_b])), consume=consume_qkv,
                  cons_in=dict(wqkv=wq_b), cons_out=qkv_out)
        qkv_b = u2["qkv_h"]
        attn_b, lse_b = attention_forward(qkv_b, head_dim, n_heads)
        u3 = unit(3, "out_mlp1", seq, width, lhs=[attn_b], weight=[wo_b], local=middle, tail=keep,
                  local_in=dict(res=u2["res_out"], ln=jnp.stack([gain_d, shift_d, bias_c])), consume=consume_up_down,
                  cons_in=dict(w_up=up_b, b_up=bup_b, dy=dy_all, w_down=down_b), cons_out=dict(act=(ff, BF16), d_pre=(ff, BF16)),
                  cons_acc=bup_acc)
        u4 = unit(4, "down_y", seq, width, lhs=[u3["act_h"]], weight=[down_b], local=leave, tail=dict(res_out=bf_rows),
                  local_in=dict(res=u3["res_out"], ln=jnp.stack([gain_d, shift_d, bias_d2])))

        u5 = unit(5, "dup_dattn1", seq, width, lhs=[u3["d_pre_h"]], weight=[up_b], weight_t=True, local=backward, tail=back,
                  local_in=dict(res=u3["res_out"], d_res=dy, ln=gain_d[None]), consume=consume_dattn,
                  cons_in=dict(w_out=wo_b), cons_out=dattn_out)
        dqkv_b = attention_backward(qkv_b, attn_b, u5["d_attn_h"], lse_b, head_dim, n_heads)
        u6 = unit(6, "dqkv_dpre0", seq, width, lhs=list(dqkv_b), weight=part_b, local=backward, tail=back,
                  local_in=dict(res=u2["res_out"], d_res=u5["d_out"], ln=gain_c[None]), consume=consume_dpre,
                  cons_in=dict(w_down=down_a, gel=u1["gel_h"]), cons_out=dict(d_pre=(ff, BF16)), cons_acc=bup_acc)
        u7 = unit(7, "dup_dattn0", seq, width, lhs=[u6["d_pre_h"]], weight=[up_a], weight_t=True, local=backward, tail=back,
                  local_in=dict(res=u1["res_out"], d_res=u6["d_out"], ln=gain_b[None]), consume=consume_dattn,
                  cons_in=dict(w_out=wo_a), cons_out=dattn_out)
        dqkv_a = attention_backward(qkv_a, attn_a, u7["d_attn_h"], lse_a, head_dim, n_heads)
        u7_sums, u6_sums, u5_sums = [u["sums"][:3] for u in (u7, u6, u5)]
        pair = jnp.zeros((2, width), F32)
        small = jnp.concatenate([pair, u7_sums, u6_sums, u5_sums, jnp.sum(dy.astype(F32), axis=0, keepdims=True), pair, pair])
        u8 = unit(8, "dqkv_dx", seq, width, lhs=list(dqkv_a), weight=part_a, local=local_backward(rows, True),
                  local_in=dict(res=x_in, d_res=u7["d_out"], ln=gain_a[None], small=small),
                  tail=dict(d_out=bf_rows, small_out=((16, width), F32)))
        g0, s0, g1, s1, b0, g2, s2, b1, g3, s3, b2, b3 = u8["small_out"][:12]
        ln_grad = jnp.stack(stack_all([[g0, s0, g1, s1], [g2, s2, g3, s3]]))
        bias_grad = jnp.stack(stack_all([[b0, b1], [b2, b3]]))

        def grads(lefts, rights):
            return [dot_tn(a, b).astype(BF16) for a, b in zip(lefts, rights)]

        def drop_pad(g):
            return g.reshape((-1, LANES, width))[:, :head_dim]

        g_down = grads([u1["act_h"], u3["act_h"]], [u6["h_all"], dy_all])
        g_up = grads([u1["h_all"], u3["h_all"]], [u6["d_pre_h"], u3["d_pre_h"]])
        g_out = [drop_pad(g) for g in grads([attn_a, attn_b], [u7["h_all"], u5["h_all"]])]
        g_qkv = [jnp.stack([drop_pad(g) for g in grads(d, [h] * len(d))])
                 for d, h in ((dqkv_a, u0["h_all"]), (dqkv_b, u2["h_all"]))]
        d_bup = [jnp.sum(u["d_bup"], axis=0) for u in (u6, u3)]
        g_qkv, g_out, g_up, d_bup, g_down = stack_all([g_qkv, g_out, g_up, d_bup, g_down])
        return (u4["res_out"][None], u8["d_out"][None], ln_grad, bias_grad, jnp.moveaxis(g_qkv, -1, 1), g_out, g_up, d_bup, g_down)

    tokens, rep = spec("dp tp ."), spec(". . .")
    in_specs = (tokens, tokens, rep, rep, spec(". . . tp ."), spec(". tp . ."), spec(". . tp"), spec(". tp"), spec(". tp ."))
    out_specs = (tokens, tokens, spec("dp . ."), spec("dp . ."), spec("dp . . tp ."), spec("dp tp . ."), spec("dp . tp"),
                 spec("dp tp"), spec("dp tp ."))
    return jax.shard_map(device_step, mesh=mesh, in_specs=in_specs, out_specs=out_specs, check_vma=False)
```

```python
import functools
import math

import jax
import jax.numpy as jnp
from jax import lax
from jax.experimental import pallas as pl
from jax.experimental.pallas import tpu as pltpu
from jax.sharding import PartitionSpec as P

MESH = pl.DeviceIdType.MESH
BF16 = jnp.bfloat16
F32 = jnp.float32
LOG2E = math.log2(math.e)
VMEM_LIMIT = 60 * 1024 * 1024
LANES = 128


def dot_nn(a, b):
    return lax.dot_general(a, b, (((1,), (0,)), ((), ())), preferred_element_type=F32)


def dot_nt(a, b):
    return lax.dot_general(a, b, (((1,), (1,)), ((), ())), preferred_element_type=F32)


def dot_tn(a, b):
    return lax.dot_general(a, b, (((0,), (0,)), ((), ())), preferred_element_type=F32)


def attn_fwd_kernel(scale, n_q, q_ref, k_ref, v_ref, a_ref, lse_ref):
    blk = q_ref.shape[0]
    coef = scale * LOG2E
    row = lax.broadcasted_iota(jnp.int32, (blk, blk), 0)
    col = lax.broadcasted_iota(jnp.int32, (blk, blk), 1)

    def variant(i):
        q = q_ref[...]
        parts = []
        for j in range(i + 1):
            s = dot_nt(q, k_ref[j * blk:(j + 1) * blk, :])
            if j == i:
                s = jnp.where(row >= col, s, -1e30)
            parts.append(s)
        top = parts[0]
        for s in parts[1:]:
            top = jnp.maximum(top, s)
        top = jnp.max(top, axis=-1, keepdims=True) * coef
        parts = [jnp.exp2(s * coef - top) for s in parts]
        total = parts[0]
        for e in parts[1:]:
            total = total + e
        total = jnp.sum(total, axis=-1, keepdims=True)
        inv = 1.0 / total
        out = None
        for j, e in enumerate(parts):
            o = dot_nn((e * inv).astype(BF16), v_ref[j * blk:(j + 1) * blk, :])
            out = o if out is None else out + o
        a_ref[...] = out.astype(BF16)
        lse = jnp.broadcast_to(top + jnp.log2(total), (blk, 128))
        lse_ref[0] = jnp.transpose(lse)[0:1, :]

    for i in range(n_q):
        pl.when(pl.program_id(1) == i)(functools.partial(variant, i))


def attention_forward(qkv, head_dim, n_heads):
    seq = qkv.shape[0]
    blk = 512
    n_q = seq // blk
    return pl.pallas_call(
        functools.partial(attn_fwd_kernel, head_dim ** -0.5, n_q),
        grid=(n_heads, n_q),
        in_specs=[pl.BlockSpec((blk, 128), lambda h, i: (i, h)),
                  pl.BlockSpec((seq, 128), lambda h, i: (0, n_heads + h)),
                  pl.BlockSpec((seq, 128), lambda h, i: (0, 2 * n_heads + h))],
        out_specs=[pl.BlockSpec((blk, 128), lambda h, i: (i, h)),
                   pl.BlockSpec((1, 1, blk), lambda h, i: (h, 0, i))],
        out_shape=[jax.ShapeDtypeStruct((seq, n_heads * 128), BF16),
                   jax.ShapeDtypeStruct((n_heads, 1, seq), F32)],
        compiler_params=pltpu.CompilerParams(dimension_semantics=("arbitrary", "arbitrary"), vmem_limit_bytes=40 * 1024 * 1024),
        cost_estimate=pl.CostEstimate(flops=4 * seq * seq * 128, bytes_accessed=8 * seq * 256, transcendentals=seq * seq),
        name="attn_fwd",
    )(qkv, qkv, qkv)


def attn_bwd_kernel(scale, n_q, q_ref, k_ref, v_ref, a_ref, da_ref, lse_ref, dq_ref, dk_ref, dv_ref, dk_acc, dv_acc):
    blk = q_ref.shape[0]
    coef = scale * LOG2E
    key = lax.broadcasted_iota(jnp.int32, (blk, blk), 0)
    qry = lax.broadcasted_iota(jnp.int32, (blk, blk), 1)

    def variant(i):
        q = q_ref[...]
        da = da_ref[...]
        lse = lse_ref[0]
        row_dot = jnp.sum(jnp.transpose(da.astype(F32) * a_ref[...].astype(F32)), axis=0, keepdims=True)
        dq = None
        for j in range(i, -1, -1):
            rows = slice(j * blk, (j + 1) * blk)
            k = k_ref[rows, :]
            p = jnp.exp2(dot_nt(k, q) * coef - lse)
            if j == i:
                p = jnp.where(qry >= key, p, 0.0)
            dv = dot_nn(p.astype(BF16), da)
            ds = (p * (dot_nt(v_ref[rows, :], da) - row_dot)).astype(BF16)
            dk = dot_nn(ds, q)
            if j == i:
                dv_acc[rows, :] = dv
                dk_acc[rows, :] = dk
            else:
                dv_acc[rows, :] += dv
                dk_acc[rows, :] += dk
            d = dot_tn(ds, k)
            dq = d if dq is None else dq + d
        dq_ref[...] = (dq * scale).astype(BF16)

    for i in range(n_q):
        pl.when(pl.program_id(1) == i)(functools.partial(variant, i))

    @pl.when(pl.program_id(1) == n_q - 1)
    def _():
        dk_ref[...] = (dk_acc[...] * scale).astype(BF16)
        dv_ref[...] = dv_acc[...].astype(BF16)


def attention_backward(qkv, attn, d_attn, lse, head_dim, n_heads):
    seq = qkv.shape[0]
    blk = 512
    n_q = seq // blk
    row = pl.BlockSpec((blk, 128), lambda h, i: (i, h))
    full = pl.BlockSpec((seq, 128), lambda h, i: (0, h))
    shape = jax.ShapeDtypeStruct((seq, n_heads * 128), BF16)
    return pl.pallas_call(
        functools.partial(attn_bwd_kernel, head_dim ** -0.5, n_q),
        grid=(n_heads, n_q),
        in_specs=[row,
                  pl.BlockSpec((seq, 128), lambda h, i: (0, n_heads + h)),
                  pl.BlockSpec((seq, 128), lambda h, i: (0, 2 * n_heads + h)),
                  row, row,
                  pl.BlockSpec((1, 1, blk), lambda h, i: (h, 0, i))],
        out_specs=[row, full, full],
        out_shape=[shape, shape, shape],
        scratch_shapes=[pltpu.VMEM((seq, 128), F32), pltpu.VMEM((seq, 128), F32)],
        compiler_params=pltpu.CompilerParams(dimension_semantics=("arbitrary", "arbitrary"), vmem_limit_bytes=40 * 1024 * 1024),
        cost_estimate=pl.CostEstimate(flops=10 * seq * seq * 128, bytes_accessed=16 * seq * 256, transcendentals=seq * seq),
        name="attn_bwd",
    )(qkv, qkv, qkv, attn, d_attn, lse)


class Place:
    def __init__(self):
        t = lax.axis_index("tp")
        self.me = t
        self.dc = 1 - 2 * (t % 2)
        self.dx = 2 - 4 * ((t // 2) % 2)
        self.dy = 4 - 8 * (t // 4)
        self.partner = t + self.dc
        self.xn = t + self.dx
        self.yn = t + self.dy


def barrier(pos):
    sem = pltpu.get_barrier_semaphore()
    for peer in (pos.partner, pos.xn, pos.yn):
        pl.semaphore_signal(sem, inc=1, device_id={"tp": peer}, device_id_type=MESH)
    pl.semaphore_wait(sem, 3)


def rdma(src, dst, sems, idx, peer):
    send, recv = sems
    return pltpu.make_async_remote_copy(src_ref=src, dst_ref=dst, send_sem=send.at[idx], recv_sem=recv.at[idx],
                                        device_id={"tp": peer}, device_id_type=MESH)


def rs_scratch(half, width):
    quarter = half // 2
    return dict(
        rs_snd=pltpu.VMEM((2, 4, half, width), BF16), rs_rcv=pltpu.VMEM((2, 4, half, width), BF16),
        rs_sum=pltpu.VMEM((2, 4, half, width), F32), rs_out=pltpu.VMEM((2, 3, half, width), BF16),
        rs_in=pltpu.VMEM((2, 6, quarter, width), BF16),
        rs_psend=pltpu.SemaphoreType.DMA((2, 4)), rs_precv=pltpu.SemaphoreType.DMA((2, 4)),
        rs_send=pltpu.SemaphoreType.DMA((2, 6)), rs_recv=pltpu.SemaphoreType.DMA((2, 6)))


class ReduceScatter:
    def __init__(self, pos, r, hf, half, width, produce, n_chunk=3):
        self.pos, self.r, self.hf, self.half, self.produce = pos, r, hf, half, produce
        self.cols = [pl.ds(c * (width // n_chunk), width // n_chunk) for c in range(n_chunk)]
        self.quarter = half // 2
        top, low = pl.ds(0, self.quarter), pl.ds(self.quarter, self.quarter)
        sems = (r.rs_send.at[hf], r.rs_recv.at[hf])

        def hop(i, slot, part, peer):
            return rdma(r.rs_out.at[hf, slot, part], r.rs_in.at[hf, i], sems, i, peer)

        self.diag_x, self.diag_y = hop(0, 0, top, pos.xn), hop(1, 0, low, pos.yn)
        self.x_top, self.x_low = hop(2, 1, top, pos.xn), hop(3, 1, low, pos.xn)
        self.y_top, self.y_low = hop(4, 2, top, pos.yn), hop(5, 2, low, pos.yn)

    def dest(self, k):
        return self.pos.me + (1 - k // 2) * self.pos.dx + (1 - k % 2) * self.pos.dy

    def to_partner(self, k):
        r, hf = self.r, self.hf
        return rdma(r.rs_snd.at[hf, k], r.rs_rcv.at[hf, k], (r.rs_psend.at[hf], r.rs_precv.at[hf]), k, self.pos.partner)

    def compute(self, send):
        r, hf = self.r, self.hf

        def first(k, carry):
            for cols in self.cols:
                r.rs_snd[hf, k, :, cols] = self.produce(self.dest(k) + self.pos.dc, cols).astype(BF16)
            self.to_partner(k).start()
            return carry

        lax.fori_loop(0, 4, first, 0)

        def second(k, carry):
            self.to_partner(k).wait_recv()
            for cols in self.cols:
                total = self.produce(self.dest(k), cols) + r.rs_rcv[hf, k, :, cols].astype(F32)
                r.rs_sum[hf, k, :, cols] = total

                @pl.when(k < 3)
                def _():
                    r.rs_out[hf, k, :, cols] = r.rs_sum[hf, k, :, cols].astype(BF16)

            if send:
                self.send(k)
            return carry

        lax.fori_loop(0, 4, second, 0)

    def send(self, k):
        @pl.when(k == 0)
        def _():
            self.diag_x.start()
            self.diag_y.start()

        @pl.when(k == 1)
        def _():
            self.x_top.start()

        @pl.when(k == 2)
        def _():
            self.y_low.start()

    def send_all(self):
        for copy in (self.diag_x, self.diag_y, self.x_top, self.y_low):
            copy.start()

    def relay(self):
        r, hf = self.r, self.hf

        def add(slot, part):
            def body(i, carry):
                rr = pl.ds(pl.multiple_of(i * 16, 16), 16)
                at = pl.ds(pl.multiple_of(part * self.quarter + i * 16, 16), 16)
                r.rs_out[hf, slot, at, :] = (r.rs_sum[hf, slot, at, :] + r.rs_in[hf, part, rr, :].astype(F32)).astype(BF16)
                return carry

            lax.fori_loop(0, self.quarter // 16, body, 0)

        self.diag_x.wait_recv()
        add(2, 0)
        self.y_top.start()
        self.diag_y.wait_recv()
        add(1, 1)
        self.x_low.start()

    def finish(self):
        for copy in (self.x_top, self.y_low, self.y_top, self.x_low):
            copy.wait_recv()

    def rows(self, start, count):
        r, hf = self.r, self.hf
        part = start // self.quarter
        inner = pl.ds(pl.multiple_of(start - part * self.quarter, count), count)
        mine = r.rs_sum[hf, 3, pl.ds(start, count), :]
        return (mine + r.rs_in[hf, 2 + part, inner, :].astype(F32)) + r.rs_in[hf, 4 + part, inner, :].astype(F32)

    def drain(self):
        for k in range(4):
            self.to_partner(k).wait_send()
        for copy in (self.diag_x, self.diag_y, self.x_top, self.x_low, self.y_top, self.y_low):
            copy.wait_send()


def ag_scratch(seq, width):
    return dict(h_vm=pltpu.VMEM((seq, width), BF16), h_out=pltpu.SemaphoreType.DMA((2, 8)),
                ag_send=pltpu.SemaphoreType.DMA((2, 13)), ag_recv=pltpu.SemaphoreType.DMA((2, 13)))


class AllGather:
    def __init__(self, pos, r, hf, half, consume, streams):
        self.pos, self.hf, self.half, self.consume, self.streams = pos, hf, half, consume, streams
        quarter = half // 2
        sems = (r.ag_send.at[hf], r.ag_recv.at[hf])
        me, xn, yn, mate = pos.me, pos.xn, pos.yn, pos.partner
        dn = me + pos.dx + pos.dy

        def copy(i, owner, part, peer):
            ref = r.h_vm.at[pl.ds(pl.multiple_of(owner * 2 * half + hf * half + part * quarter, quarter), quarter)]
            return rdma(ref, ref, sems, i, peer)

        ref = r.h_vm.at[pl.ds(pl.multiple_of(me * 2 * half + hf * half, half), half)]
        self.own_p = rdma(ref, ref, sems, 0, mate)
        self.own_xa, self.own_xb = copy(1, me, 0, xn), copy(2, me, 1, xn)
        self.own_ya, self.own_yb = copy(3, me, 0, yn), copy(4, me, 1, yn)
        self.relay_y = copy(5, xn, 0, yn)
        self.relay_x = copy(6, yn, 1, xn)
        self.fwd_xa, self.fwd_xb = copy(7, xn, 0, mate), copy(8, xn, 1, mate)
        self.fwd_ya, self.fwd_yb = copy(9, yn, 0, mate), copy(10, yn, 1, mate)
        self.fwd_da, self.fwd_db = copy(11, dn, 0, mate), copy(12, dn, 1, mate)

    def start(self):
        for copy in (self.own_xa, self.own_yb, self.own_xb, self.own_ya, self.own_p):
            copy.start()

    def relay(self):
        self.own_xa.wait_recv()
        self.relay_y.start()
        self.fwd_xa.start()
        self.own_yb.wait_recv()
        self.relay_x.start()
        self.fwd_yb.start()

    def second(self):
        self.own_xb.wait_recv()
        self.fwd_xb.start()
        self.own_ya.wait_recv()
        self.fwd_ya.start()

    def last(self):
        self.relay_y.wait_recv()
        self.fwd_da.start()
        self.relay_x.wait_recv()
        self.fwd_db.start()

    def out_copies(self, s):
        pos = self.pos
        block = pos.me + (s % 2) * pos.dc + ((s // 2) % 2) * pos.dx + (s // 4) * pos.dy
        at = pl.ds(pl.multiple_of(block * 2 * self.half + self.hf * self.half, self.half), self.half)
        return at, [pltpu.make_async_copy(src.at[at], dst.at[at], sem.at[self.hf, s]) for src, dst, sem in self.streams]

    def use(self, first, until):
        def step(s, carry):
            @pl.when(s == 1)
            def _():
                self.own_p.wait_recv()

            @pl.when(s == 3)
            def _():
                self.fwd_xa.wait_recv()
                self.fwd_xb.wait_recv()

            @pl.when(s == 5)
            def _():
                self.fwd_ya.wait_recv()
                self.fwd_yb.wait_recv()

            @pl.when(s == 7)
            def _():
                self.fwd_da.wait_recv()
                self.fwd_db.wait_recv()

            at, copies = self.out_copies(s)
            self.consume(at)
            for c in copies:
                c.start()
            return carry

        lax.fori_loop(first, until, step, 0)

    def drain(self):
        for c in (self.own_p, self.own_xa, self.own_xb, self.own_ya, self.own_yb, self.relay_y, self.relay_x, self.fwd_xa,
                  self.fwd_xb, self.fwd_ya, self.fwd_yb, self.fwd_da, self.fwd_db):
            c.wait_send()

        def body(s, carry):
            for c in self.out_copies(s)[1]:
                c.wait()
            return carry

        lax.fori_loop(0, 8, body, 0)


class Refs:
    pass


def comm_call(body, ins, outs, scratch, cid, name, flops):
    in_names, out_names, scr_names = list(ins), list(outs), list(scratch)
    any_spec, vmem_spec = pl.BlockSpec(memory_space=pl.ANY), pl.BlockSpec(memory_space=pltpu.VMEM)
    arrays, in_specs = [], []
    for key in in_names:
        val = ins[key]
        in_specs.append(any_spec if isinstance(val, tuple) else vmem_spec)
        arrays.append(val[0] if isinstance(val, tuple) else val)

    def kernel(*refs):
        r = Refs()
        for key, ref in zip(in_names + out_names + scr_names, refs):
            setattr(r, key, ref)
        body(r)

    result = pl.pallas_call(
        kernel,
        in_specs=in_specs,
        out_specs=[any_spec if outs[key][2] else vmem_spec for key in out_names],
        out_shape=[jax.ShapeDtypeStruct(outs[key][0], outs[key][1]) for key in out_names],
        scratch_shapes=[scratch[key] for key in scr_names],
        compiler_params=pltpu.CompilerParams(collective_id=cid, has_side_effects=True, vmem_limit_bytes=VMEM_LIMIT),
        cost_estimate=pl.CostEstimate(flops=flops, bytes_accessed=30_000_000, transcendentals=0),
        name=name,
    )(*arrays)
    return dict(zip(out_names, result))


def fold8(vals):
    out = vals[0:8]
    for i in range(8, vals.shape[0], 8):
        out = out + vals[i:i + 8]
    return out


class Stage:
    def __init__(self, local, local_in, local_out=None, lhs=(), weight=(), weight_t=False, consume=None, cons_in=None,
                 cons_out=None, cons_acc=None, after=None):
        self.local, self.local_in, self.local_out = local, local_in, local_out or {}
        self.lhs, self.weight, self.weight_t = lhs, weight, weight_t
        self.consume, self.cons_in, self.cons_out, self.cons_acc = consume, cons_in or {}, cons_out or {}, cons_acc or {}
        self.after = after


def segment(cid, name, seq, width, stages, extra=None):
    rows = seq // 8
    half = rows // 2
    ins, outs, scratch = {}, {}, dict(extra or {})
    loads = []
    alias = [{} for _ in stages]

    def load(i, key, arr):
        tag = f"s{i}_{key}"
        ins[tag + "_h"] = (arr,)
        scratch[tag] = pltpu.VMEM(arr.shape, arr.dtype)
        loads.append(tag)
        alias[i][key] = tag

    flops = 100_000
    for i, st in enumerate(stages):
        for j, w in enumerate(st.weight):
            load(i, f"w{j}", w)
            if isinstance(st.lhs, str):
                alias[i]["lhs0"] = alias[i - 1][st.lhs]
            else:
                load(i, f"lhs{j}", st.lhs[j])
            flops += 2 * seq * width * LANES * 2
        for key, val in st.local_in.items():
            if isinstance(val, str):
                alias[i][key] = alias[i - 1][val]
            else:
                ins[f"s{i}_{key}"] = val
                alias[i][key] = f"s{i}_{key}"
        for key, (shape, dtype) in st.local_out.items():
            outs[f"s{i}_{key}"] = (shape, dtype, False)
            alias[i][key] = f"s{i}_{key}"
        if st.weight:
            scratch.update(rs_scratch(half, width))
        if st.consume:
            scratch.update(ag_scratch(seq, width))
            for key, arr in st.cons_in.items():
                load(i, key, arr)
            outs[f"s{i}_h_all"] = ((seq, width), BF16, True)
            for key, (cols, dtype) in st.cons_out.items():
                tag = f"s{i}_{key}"
                outs[tag + "_h"] = ((seq, cols), dtype, True)
                scratch[tag] = pltpu.VMEM((seq, cols), dtype)
                scratch[tag + "_s"] = pltpu.SemaphoreType.DMA((2, 8))
                alias[i][key] = tag
                flops += 2 * seq * width * cols
            for key, (shape, dtype) in st.cons_acc.items():
                outs[f"s{i}_{key}"] = (shape, dtype, False)
                alias[i][key] = f"s{i}_{key}"
    scratch["load_sem"] = pltpu.SemaphoreType.DMA((len(loads),))

    def body(r):
        pos = Place()
        pending = {}
        for n, tag in enumerate(loads):
            pending[tag] = pltpu.make_async_copy(getattr(r, tag + "_h"), getattr(r, tag), r.load_sem.at[n])
            pending[tag].start()

        def need(i, keys):
            for key in keys:
                copy = pending.pop(alias[i].get(key), None)
                if copy is not None:
                    copy.wait()

        barrier(pos)
        rs, ag, views = [], [], []
        for i, st in enumerate(stages):
            v = Refs()
            for key, tag in alias[i].items():
                setattr(v, key, getattr(r, tag))
            for key in scratch:
                if key.startswith(("h_", "sm_")):
                    setattr(v, key, getattr(r, key))
            views.append(v)
            pairs = [(f"lhs{j}", f"w{j}") for j in range(len(st.weight))]

            def produce(hf, block, cols, v=v, st=st, pairs=pairs):
                at = pl.ds(pl.multiple_of(block * rows + hf * half, half), half)
                total = None
                for a, w in pairs:
                    a, w = getattr(v, a), getattr(v, w)
                    part = dot_nt(a[at, :], w[cols, :]) if st.weight_t else dot_nn(a[at, :], w[:, cols])
                    total = part if total is None else total + part
                return total

            rs.append([ReduceScatter(pos, r, hf, half, width, functools.partial(produce, hf)) for hf in range(2)]
                      if st.weight else None)
            if st.consume:
                streams = [(r.h_vm, getattr(r, f"s{i}_h_all"), r.h_out)]
                for key in st.cons_out:
                    tag = alias[i][key]
                    streams.append((getattr(r, tag), getattr(r, tag + "_h"), getattr(r, tag + "_s")))
                ag.append([AllGather(pos, r, hf, half, functools.partial(st.consume, v), streams) for hf in range(2)])
            else:
                ag.append(None)

        def local(i, hf):
            reduced = None
            if rs[i]:
                rs[i][hf].finish()
                reduced = rs[i][hf].rows
            stages[i].local(views[i], pos, hf, half, reduced)
            if rs[i]:
                rs[i][hf].drain()
            if ag[i]:
                ag[i][hf].start()

        def front(i, hf):
            need(i, [f"{kind}{j}" for j in range(len(stages[i].weight)) for kind in ("lhs", "w")])
            rs[i][hf].compute(send=hf == 0)

        for i, st in enumerate(stages):
            before = ag[i - 1] if i else None
            if rs[i]:
                if before:
                    before[0].drain()
                front(i, 0)
            if before:
                before[1].use(0, 2)
                before[1].second()
                before[1].use(2, 6)
                before[1].last()
                before[1].use(6, 8)
                before[1].drain()
            if rs[i]:
                front(i, 1)
                rs[i][0].relay()
                rs[i][1].send_all()
            if ag[i]:
                need(i, list(st.cons_in))
                for key in st.cons_acc:
                    ref = getattr(views[i], key)
                    ref[...] = jnp.zeros_like(ref)
            local(i, 0)
            if rs[i]:
                if ag[i]:
                    ag[i][0].use(0, 2)
                rs[i][1].relay()
            local(i, 1)
            if ag[i]:
                ag[i][0].relay()
                if not rs[i]:
                    ag[i][0].use(0, 2)
                ag[i][0].second()
                ag[i][0].use(2, 6)
                ag[i][1].relay()
                ag[i][0].last()
                ag[i][0].use(6, 8)
        if ag[-1]:
            ag[-1][1].use(0, 2)
            ag[-1][1].second()
            ag[-1][1].use(2, 6)
            ag[-1][1].last()
            ag[-1][1].use(6, 8)
            for one in ag[-1]:
                one.drain()
        if stages[-1].after:
            stages[-1].after(views[-1], pos)

    res = comm_call(body, ins, outs, scratch, cid, name, flops)
    made = []
    for i in range(len(stages)):
        tag = f"s{i}_"
        made.append({key[len(tag):].removesuffix("_h"): val for key, val in res.items() if key.startswith(tag)})
    return made


STEP_ROWS = 16


def normalize(res):
    mean = jnp.mean(res, axis=-1, keepdims=True)
    centered = res - mean
    var = jnp.mean(centered * centered, axis=-1, keepdims=True)
    rstd = lax.rsqrt(var + 1e-5)
    return centered * rstd, rstd


def local_forward(with_sum, with_h):
    def run(v, pos, hf, half, reduced):
        def step(i, carry):
            inner = pl.multiple_of(i * STEP_ROWS, STEP_ROWS)
            at = pl.multiple_of(hf * half + inner, STEP_ROWS)
            here = pl.ds(at, STEP_ROWS)
            res = v.res[here, :].astype(F32)
            if with_sum:
                res = (res + reduced(inner, STEP_ROWS)) + v.ln[2:, :]
                v.res_out[here, :] = res.astype(v.res_out.dtype)
            if with_h:
                xhat, _ = normalize(res)
                v.h_vm[pl.ds(pl.multiple_of(pos.me * 2 * half + at, STEP_ROWS), STEP_ROWS), :] = (
                    xhat * v.ln[0:1, :] + v.ln[1:2, :]).astype(BF16)
            return carry

        lax.fori_loop(0, half // STEP_ROWS, step, 0)

    return run


def local_backward(last):
    def run(v, pos, hf, half, reduced):
        def step(i, carry):
            d_gain, d_shift, d_bias = carry
            inner = pl.multiple_of(i * STEP_ROWS, STEP_ROWS)
            at = pl.multiple_of(hf * half + inner, STEP_ROWS)
            here = pl.ds(at, STEP_ROWS)
            d_h = reduced(inner, STEP_ROWS)
            xhat, rstd = normalize(v.res[here, :].astype(F32))
            d_gain = d_gain + fold8(d_h * xhat)
            d_shift = d_shift + fold8(d_h)
            d_hat = d_h * v.ln[0:1, :]
            m_one = jnp.mean(d_hat, axis=-1, keepdims=True)
            m_two = jnp.mean(d_hat * xhat, axis=-1, keepdims=True)
            d_out = v.d_res[here, :].astype(F32) + rstd * (d_hat - m_one - xhat * m_two)
            d_bias = d_bias + fold8(d_out)
            v.d_out[here, :] = d_out.astype(v.d_out.dtype)
            if not last:
                v.h_vm[pl.ds(pl.multiple_of(pos.me * 2 * half + at, STEP_ROWS), STEP_ROWS), :] = d_out.astype(BF16)
            return d_gain, d_shift, d_bias

        zero = jnp.zeros((8, v.ln.shape[-1]), F32)
        totals = lax.fori_loop(0, half // STEP_ROWS, step, (zero, zero, zero))
        for n, total in enumerate(totals):
            row = slice(n, n + 1)
            total = jnp.sum(total, axis=0, keepdims=True)
            v.sums[row, :] = v.sums[row, :] + total if hf else total

    return run


def small_scratch(width):
    shape = (3, 16, width)
    return dict(sm_snd=pltpu.VMEM(shape, F32), sm_rcv=pltpu.VMEM(shape, F32), sm_send=pltpu.SemaphoreType.DMA((3,)),
                sm_recv=pltpu.SemaphoreType.DMA((3,)))


def small_sum(v, pos):
    v.sm_snd[0] = v.small[...]
    v.sm_snd[0, 0:2, :] = v.sums[0:2, :]
    sems = (v.sm_send, v.sm_recv)
    copies = []
    for i, peer in enumerate((pos.partner, pos.xn, pos.yn)):
        c = rdma(v.sm_snd.at[i], v.sm_rcv.at[i], sems, i, peer)
        c.start()
        c.wait_recv()
        copies.append(c)
        total = v.sm_snd[i] + v.sm_rcv[i]
        if i < 2:
            v.sm_snd[i + 1] = total
        else:
            v.small_out[...] = total
    for c in copies:
        c.wait_send()


GELU_C = math.sqrt(2.0 / math.pi)


def gelu_pair(x):
    sq = x * x
    t = jnp.tanh(GELU_C * x * (1.0 + 0.044715 * sq))
    half = 0.5 * (1.0 + t)
    grad = half + (0.5 * GELU_C) * x * (1.0 - t * t) * (1.0 + (3 * 0.044715) * sq)
    return x * half, grad


def consume_qkv(r, at):
    h = r.h_vm[at, :]
    for c in range(0, r.qkv.shape[1], 256):
        cols = pl.ds(c, 256)
        r.qkv[at, cols] = dot_nt(h, r.wqkv[cols, :]).astype(BF16)


def consume_up(r, at):
    h = r.h_vm[at, :]
    for c in range(0, r.act.shape[1], 256):
        cols = pl.ds(c, 256)
        act, grad = gelu_pair(dot_nn(h, r.w_up[:, cols]) + r.b_up[:, cols])
        r.act[at, cols] = act.astype(BF16)
        r.gel[at, cols] = grad


def consume_up_down(r, at):
    h = r.h_vm[at, :]
    dy = r.dy[at, :]
    for c in range(0, r.act.shape[1], 256):
        cols = pl.ds(c, 256)
        act, grad = gelu_pair(dot_nn(h, r.w_up[:, cols]) + r.b_up[:, cols])
        r.act[at, cols] = act.astype(BF16)
        d_pre = dot_nt(dy, r.w_down[cols, :]) * grad
        r.d_bup[:, cols] += fold8(d_pre)
        r.d_pre[at, cols] = d_pre.astype(BF16)


def consume_dpre(r, at):
    d = r.h_vm[at, :]
    for c in range(0, r.d_pre.shape[1], 256):
        cols = pl.ds(c, 256)
        d_pre = dot_nt(d, r.w_down[cols, :]) * r.gel[at, cols]
        r.d_bup[:, cols] += fold8(d_pre)
        r.d_pre[at, cols] = d_pre.astype(BF16)


def consume_dattn(r, at):
    r.d_attn[at, :] = dot_nt(r.h_vm[at, :], r.w_out[...]).astype(BF16)


def spec(text):
    return P(*[dict(d="dp", t="tp").get(letter) for letter in text])


def stack_all(groups):
    return [jnp.stack(group) for group in groups]


def solution(mesh):
    def device_step(x_loc, dy_loc, ln_par, bias_d, w_qkv, w_out, w_up, b_up, w_down):
        (x_in,), (dy,) = x_loc, dy_loc
        rows, width = x_in.shape
        seq = rows * mesh.shape['tp']
        n_heads, head_dim = w_qkv.shape[-2:]
        ff = w_up.shape[-1]
        lanes = n_heads * LANES

        def pad_heads(w):
            flat = w.reshape((-1, head_dim, width))
            return jnp.concatenate([flat, jnp.zeros((flat.shape[0], LANES - head_dim, width), BF16)], axis=1).reshape((-1, width))

        wqkv_t = [pad_heads(jnp.moveaxis(w, 0, -1)) for w in w_qkv]
        wo = [pad_heads(w) for w in w_out]
        parts = [w.reshape((-1, lanes, width)) for w in wqkv_t]
        (up_a, up_b), (down_a, down_b), (wq_a, wq_b), (wo_a, wo_b) = w_up, w_down, wqkv_t, wo
        bup_a, bup_b = jnp.split(b_up, 2)
        (gain_a, shift_a, gain_b, shift_b), (gain_c, shift_c, gain_d, shift_d) = ln_par
        (bias_a, bias_b), (bias_c, bias_d2) = bias_d
        part_a, part_b = [list(w) for w in parts]

        f32_rows = ((rows, width), F32)
        bf_rows = ((rows, width), BF16)
        sums = ((8, width), F32)
        keep = dict(res_out=f32_rows)
        back = dict(d_out=f32_rows, sums=sums)
        qkv_out = dict(qkv=(len(wq_a), BF16))
        dattn_out = dict(d_attn=(lanes, BF16))
        bup_acc = dict(d_bup=((8, ff), F32))
        enter, middle, leave = local_forward(False, True), local_forward(True, True), local_forward(True, False)
        backward = local_backward(False)
        act_out = dict(act=(ff, BF16))

        (u0,) = segment(0, "ag_qkv", seq, width, [Stage(
            enter, dict(res=x_in, ln=jnp.stack([gain_a, shift_a])), consume=consume_qkv, cons_in=dict(wqkv=wq_a), cons_out=qkv_out)])
        qkv_a = u0["qkv"]
        dy_dep, _ = lax.optimization_barrier((dy, qkv_a))
        dy_all = lax.all_gather(dy_dep, 'tp', axis=0, tiled=True)

        attn_a, lse_a = attention_forward(qkv_a, head_dim, n_heads)
        u1, u2 = segment(1, "mid_fwd", seq, width, [
            Stage(middle, dict(res=x_in, ln=jnp.stack([gain_b, shift_b, bias_a])), keep, lhs=[attn_a], weight=[wo_a],
                  consume=consume_up, cons_in=dict(w_up=up_a, b_up=bup_a), cons_out=dict(act_out, gel=(ff, F32))),
            Stage(middle, dict(res="res_out", ln=jnp.stack([gain_c, shift_c, bias_b])), keep, lhs="act", weight=[down_a],
                  consume=consume_qkv, cons_in=dict(wqkv=wq_b), cons_out=qkv_out)])
        qkv_b = u2["qkv"]
        attn_b, lse_b = attention_forward(qkv_b, head_dim, n_heads)
        u3, u5 = segment(2, "turn", seq, width, [
            Stage(middle, dict(res=u2["res_out"], ln=jnp.stack([gain_d, shift_d, bias_c])), keep, lhs=[attn_b], weight=[wo_b],
                  consume=consume_up_down, cons_in=dict(w_up=up_b, b_up=bup_b, dy=dy_all, w_down=down_b),
                  cons_out=dict(act_out, d_pre=(ff, BF16)), cons_acc=bup_acc),
            Stage(backward, dict(res="res_out", d_res=dy, ln=gain_d[None]), back, lhs="d_pre", weight=[up_b], weight_t=True,
                  consume=consume_dattn, cons_in=dict(w_out=wo_b), cons_out=dattn_out)])
        (u4,) = segment(3, "down_y", seq, width, [Stage(
            leave, dict(res=u3["res_out"], ln=jnp.stack([gain_d, shift_d, bias_d2])), dict(res_out=bf_rows), lhs=[u3["act"]],
            weight=[down_b])])
        dqkv_b = attention_backward(qkv_b, attn_b, u5["d_attn"], lse_b, head_dim, n_heads)
        u6, u7 = segment(4, "mid_bwd", seq, width, [
            Stage(backward, dict(res=u2["res_out"], d_res=u5["d_out"], ln=gain_c[None]), back, lhs=list(dqkv_b), weight=part_b,
                  consume=consume_dpre, cons_in=dict(w_down=down_a, gel=u1["gel"]), cons_out=dict(d_pre=(ff, BF16)),
                  cons_acc=bup_acc),
            Stage(backward, dict(res=u1["res_out"], d_res="d_out", ln=gain_b[None]), back, lhs="d_pre", weight=[up_a],
                  weight_t=True, consume=consume_dattn, cons_in=dict(w_out=wo_a), cons_out=dattn_out)])
        dqkv_a = attention_backward(qkv_a, attn_a, u7["d_attn"], lse_a, head_dim, n_heads)
        u7_sums, u6_sums, u5_sums = [u["sums"][:3] for u in (u7, u6, u5)]
        pair = jnp.zeros((2, width), F32)
        small = jnp.concatenate([pair, u7_sums, u6_sums, u5_sums, jnp.sum(dy.astype(F32), axis=0, keepdims=True), pair, pair])
        (u8,) = segment(5, "end_bwd", seq, width, [Stage(
            local_backward(True), dict(res=x_in, d_res=u7["d_out"], ln=gain_a[None], small=small),
            dict(d_out=bf_rows, sums=sums, small_out=((16, width), F32)), lhs=list(dqkv_a), weight=part_a, after=small_sum)],
            small_scratch(width))
        g0, s0, g1, s1, b0, g2, s2, b1, g3, s3, b2, b3 = u8["small_out"][:12]
        ln_grad = jnp.stack(stack_all([[g0, s0, g1, s1], [g2, s2, g3, s3]]))
        bias_grad = jnp.stack(stack_all([[b0, b1], [b2, b3]]))

        def grads(lefts, rights):
            return [dot_tn(a, b).astype(BF16) for a, b in zip(lefts, rights)]

        def drop_pad(g):
            return g.reshape((-1, LANES, width))[:, :head_dim]

        g_down = grads([u1["act"], u3["act"]], [u6["h_all"], dy_all])
        g_up = grads([u1["h_all"], u3["h_all"]], [u6["d_pre"], u3["d_pre"]])
        g_out = [drop_pad(g) for g in grads([attn_a, attn_b], [u7["h_all"], u5["h_all"]])]
        g_qkv = [jnp.stack([drop_pad(g) for g in grads(d, [h] * len(d))])
                 for d, h in ((dqkv_a, u0["h_all"]), (dqkv_b, u2["h_all"]))]
        d_bup = [jnp.sum(u["d_bup"], axis=0) for u in (u6, u3)]
        g_qkv, g_out, g_up, d_bup, g_down = stack_all([g_qkv, g_out, g_up, d_bup, g_down])
        return (u4["res_out"][None], u8["d_out"][None], ln_grad, bias_grad, jnp.moveaxis(g_qkv, -1, 1), g_out, g_up, d_bup, g_down)

    tokens, rep = spec("dtn"), spec("nnn")
    in_specs = (tokens, tokens, rep, rep, spec("nnntn"), spec("ntnn"), spec("nnt"), spec("nt"), spec("ntn"))
    out_specs = (tokens, tokens, spec("dnn"), spec("dnn"), spec("dnntn"), spec("dtnn"), spec("dnt"), spec("dt"), spec("dtn"))
    return jax.shard_map(device_step, mesh=mesh, in_specs=in_specs, out_specs=out_specs, check_vma=False)
```
